32 devices in a mesh: parts: 2 (over x), rows: 16 (over z, y, core).
Axes of the slice: x: 2, y: 2, z: 4, core: 2. Of those that a mesh axis runs over, the one named last changes fastest.
Arguments:
- features: bfloat16 [128, 256, 512], P(('parts', 'rows')), parts along dimension 0, may hold values from -10 to 10, as said below
- grad_out: bfloat16 [128, 256, 512], P(('parts', 'rows')), parts along dimension 0, may hold values from -11 to 11, as said below
- filters: bfloat16 [512, 3, 3, 512], replicated, may hold values from -0.09375 to 0.09375
- norm_gain: float32 [512], replicated, may hold values from 0.25 to 1.75
- norm_bias: float32 [512], replicated, may hold values from -1 to 1
Outputs:
- grad_in: bfloat16 [128, 256, 512], P(('parts', 'rows')), parts along dimension 0
- filter_grad: float32 [1024, 3, 3, 512], P(('parts', 'rows')), parts along dimension 0
- gain_grad: float32 [1024], P('parts'), parts along dimension 0
- bias_grad: float32 [1024], P('parts'), parts along dimension 0
The draws below stay inside these ranges and needn't reach their ends.
There are 2 independent parts, one for each index of `parts`. The reference program is written for one: setup_inputs(seed, part) draws one part's arguments, and reference() takes and returns one part's arrays. A program takes and returns all parts, laid end to end along the dimension named above; an argument that names none is the same for every part. Nothing has to cross between parts.
Inputs may be any that keep to these rules, and one draw needn't show every extreme that they name: `features`: each image row has its own offset and spread for each group. `grad_out`: each image row and channel has its own offset.
All inputs are finite; a program needn't handle non-finite values.
Results may differ from the reference program's by a relative error of at most 0.0005.
Values may be sent and summed in bfloat16 or wider, within the bound.
A program may use at most 128 MiB of HBM per device.

```python
import math
import jax
import jax.numpy as jnp
from jax import lax

C = 512
GROUPS = 32
COLS = 256
HEIGHT = 64


def draw_features(key, part):
    key_noise = jax.random.fold_in(key, 11)
    key_offset = jax.random.fold_in(key, 12)
    key_spread = jax.random.fold_in(key, 13)
    normal_draw = jnp.clip(jax.random.normal(key_noise, (HEIGHT, COLS, C), jnp.float32), -4.0, 4.0)
    offset = jax.random.uniform(key_offset, (HEIGHT, 1, GROUPS), jnp.float32, -1.0, 1.0)
    spread = jnp.exp(jax.random.uniform(key_spread, (HEIGHT, 1, GROUPS), jnp.float32, math.log(0.5), math.log(2.0)))
    offset = jnp.repeat(offset, C // GROUPS, axis=2)
    spread = jnp.repeat(spread, C // GROUPS, axis=2)
    return (offset + spread * normal_draw).astype(jnp.bfloat16)


def draw_grad_out(key, part):
    key_noise = jax.random.fold_in(key, 21)
    key_offset = jax.random.fold_in(key, 22)
    normal_draw = jnp.clip(jax.random.normal(key_noise, (HEIGHT, COLS, C), jnp.float32), -4.0, 4.0)
    offset = jax.random.uniform(key_offset, (HEIGHT, 1, C), jnp.float32, -1.0, 3.0)
    return (offset + normal_draw).astype(jnp.bfloat16)


def centred(own_key, shape, scale, limit, held_as=jnp.bfloat16):
    entries = scale * jax.random.normal(own_key, shape, jnp.float32)
    return jnp.clip(entries, min=-limit, max=limit).astype(held_as)


def setup_inputs(seed: int = 0, part: int = 0) -> dict:
    streams_of = jax.random.split(jax.random.key(seed), 6)
    part_splits = jax.random.split(jax.random.fold_in(streams_of[5], part), 6)
    features = draw_features(jax.random.fold_in(jax.random.fold_in(streams_of[5], part), 71), part)
    grad_out = draw_grad_out(jax.random.fold_in(jax.random.fold_in(streams_of[5], part), 71), part)
    filters = centred(streams_of[2], (C, 3, 3, C), (9 * C) ** -0.5, 0.09375)
    norm_gain = jnp.clip(1.0 + 0.15 * jax.random.normal(streams_of[3], (C,), jnp.float32), 0.25, 1.75)
    norm_bias = jnp.clip(jax.random.uniform(streams_of[4], (C,), jnp.float32, -1.0, 1.0), -1.0, 1.0)
    return dict(features=features, grad_out=grad_out, filters=filters, norm_gain=norm_gain, norm_bias=norm_bias)


epsilon = 1e-06

def expand(values, channels):
    groups = values.shape[0]
    return jnp.broadcast_to(values[:, None], (groups, channels // groups)).reshape(channels)

def group_total(values):
    return values.reshape(GROUPS, -1).sum(axis=1)

def reference(features, grad_out, filters, norm_gain, norm_bias):
    height, columns, channels = features.shape
    pixels = height * columns
    members = pixels * (channels // GROUPS)
    widened = features.astype(jnp.float32)
    group_mean = group_total(lax.optimization_barrier(jnp.sum(widened, axis=(0, 1)))) / members
    centered = widened - expand(group_mean, channels)
    group_var = group_total(lax.optimization_barrier(jnp.sum(centered * centered, axis=(0, 1)))) / members
    inv_std = lax.rsqrt(group_var + epsilon)
    normalized = centered * expand(inv_std, channels)
    normed = normalized * norm_gain + norm_bias
    sigmoid_z = jax.nn.sigmoid(normed)
    activation = (normed * sigmoid_z).astype(jnp.bfloat16)
    flat_act = activation.reshape(-1, channels)
    padded = jnp.pad(grad_out, ((1, 1), (1, 1), (0, 0)))
    grad_act = jnp.zeros((pixels, channels), jnp.float32)
    pieces = []
    for tap_row in range(3):
        for tap_col in range(3):
            window = padded[2 - tap_row:2 - tap_row + height, 2 - tap_col:2 - tap_col + columns].reshape(-1, channels)
            grad_act = grad_act + jnp.dot(window, filters[:, tap_row, tap_col, :], preferred_element_type=jnp.float32)
            pieces.append(lax.dot_general(window, flat_act, (((0,), (0,)), ((), ())), preferred_element_type=jnp.float32))
    filter_grad = jnp.stack(pieces, axis=1).reshape(channels, 3, 3, channels) / pixels
    grad_pre = grad_act.reshape(height, columns, channels) * (sigmoid_z * (1.0 + normed * (1.0 - sigmoid_z)))
    bias_grad = lax.optimization_barrier(jnp.sum(grad_pre, axis=(0, 1)))
    gain_grad = lax.optimization_barrier(jnp.sum(grad_pre * normalized, axis=(0, 1)))
    mean_grad = group_total(norm_gain * bias_grad) / members
    mean_cross = group_total(norm_gain * gain_grad) / members
    grad_in = expand(inv_std, channels) * (grad_pre * norm_gain - expand(mean_grad, channels) - normalized * expand(mean_cross, channels))
    return (grad_in.astype(jnp.bfloat16), filter_grad, gain_grad, bias_grad)
```

```python
import functools
import math

import jax
import jax.numpy as jnp
from jax import lax
from jax.experimental import pallas as pl
from jax.experimental.pallas import tpu as pltpu
from jax.sharding import PartitionSpec as P

GROUPS = 32
LANES = 128
POWER = 9
EPSILON = 1e-06
GAIN_MAX = 1.75
BIAS_MAX = 1.0
MESH = pl.DeviceIdType.MESH
F32 = jnp.float32
BF16 = jnp.bfloat16


def encode(value):
    square = value * value
    fourth = square * square
    return (fourth * fourth * value).astype(BF16)


def decode(coded):
    wide = coded.astype(F32)
    root = jnp.exp2(jnp.log2(jnp.maximum(jnp.abs(wide), 1e-38)) * (1.0 / POWER))
    root = jnp.where(jnp.abs(wide) < 1e-37, 0.0, root)
    return jnp.where(wide < 0.0, -root, root)


def group_sum(row, per_group):
    value = jnp.broadcast_to(row, (8, LANES))
    lane = lax.broadcasted_iota(jnp.int32, (8, LANES), 1)
    step = 1
    while step < per_group:
        low = pltpu.roll(value, step, 1)
        high = pltpu.roll(value, LANES - step, 1)
        value = value + jnp.where((lane & step) != 0, low, high)
        step *= 2
    return value[0:1]


def kernel(
    n, height, width, channels,
    feat_hbm, gout_hbm, filt_hbm, gain_ref, bias_ref,
    gin_ref, fg_ref, sums_ref,
    feat, gext, filt, gt, act, gact, part, r1, s2, r2, s3, r3, stat, sums,
    local_sem, halo_send, halo_recv, stat_send, stat_recv, sums_send, sums_recv,
    send1, recv1, send2, recv2, send3, recv3,
):
    me = lax.axis_index("rows")
    core, second, third = lax.rem(me, 2), lax.rem(lax.div(me, 2), 2), lax.div(me, 4)
    thirds = n // 4
    block = channels // n
    chunks = channels // LANES
    per_group = channels // GROUPS
    local_pixels = height * width
    pixels = local_pixels * n
    members = pixels * per_group
    taps = 9

    def remote(src, dst, send, recv, target):
        return pltpu.make_async_remote_copy(
            src_ref=src, dst_ref=dst, send_sem=send, recv_sem=recv,
            device_id={"rows": target}, device_id_type=MESH,
        )

    def peer(k):
        return lax.rem(me + k, n)

    in_feat = pltpu.make_async_copy(feat_hbm, feat, local_sem.at[0])
    in_gout = pltpu.make_async_copy(
        gout_hbm, gext.at[pl.ds(width, local_pixels)], local_sem.at[1]
    )
    in_filt = pltpu.make_async_copy(filt_hbm, filt, local_sem.at[2])
    in_feat.start()
    in_gout.start()
    in_filt.start()

    barrier = pltpu.get_barrier_semaphore()

    def greet(k, carry):
        pl.semaphore_signal(barrier, inc=1, device_id={"rows": peer(k)}, device_id_type=MESH)
        return carry

    lax.fori_loop(1, n, greet, 0)

    lane = lax.broadcasted_iota(jnp.int32, (1, LANES), 1)
    slot = lane & (per_group - 1)
    in_feat.wait()
    in_gout.wait()

    packed = jnp.zeros((1, LANES), F32)
    largest = jnp.zeros((8, LANES), F32)
    for c in range(chunks):
        cols = slice(c * LANES, (c + 1) * LANES)

        def stats_step(h, carry):
            total, square, top = carry
            x = feat[pl.ds(h * width, width), cols].astype(F32)
            g = gext[pl.ds((h + 1) * width, width), cols].astype(F32)
            x = x.reshape(width // 8, 8, LANES)
            g = jnp.abs(g).reshape(width // 8, 8, LANES)
            return (
                total + x.sum(0), square + (x * x).sum(0), jnp.maximum(top, g.max(0))
            )

        zero = jnp.zeros((8, LANES), F32)
        total, square, largest = lax.fori_loop(0, height, stats_step, (zero, zero, largest))
        total = group_sum(total.sum(0, keepdims=True), per_group)
        square = group_sum(square.sum(0, keepdims=True), per_group)
        packed = packed + jnp.where(slot == c, total, 0.0)
        packed = packed + jnp.where(slot == chunks + c, square, 0.0)
    top = jnp.max(largest.max(0, keepdims=True), axis=1, keepdims=True)
    is_top = slot == 2 * chunks
    stat[me] = packed + jnp.where(is_top, top, 0.0)

    pl.semaphore_wait(barrier, n - 1)

    def stat_copy(k, source):
        return remote(stat.at[me], stat.at[source], stat_send.at[k], stat_recv.at[source], peer(k))

    def stat_start(k, carry):
        stat_copy(k, me).start()
        return carry

    lax.fori_loop(1, n, stat_start, 0)

    up, down = lax.rem(me + n - 1, n), lax.rem(me + 1, n)
    above, below = pl.ds(0, width), pl.ds((height + 1) * width, width)
    halo_up = remote(
        gext.at[pl.ds(width, width)], gext.at[below], halo_send.at[0], halo_recv.at[0], up
    )
    halo_down = remote(
        gext.at[pl.ds(height * width, width)], gext.at[above], halo_send.at[1], halo_recv.at[1], down
    )

    @pl.when(me > 0)
    def _():
        halo_up.start()

    @pl.when(me < n - 1)
    def _():
        halo_down.start()

    @pl.when(me == 0)
    def _():
        gext[above, :] = jnp.zeros((width, channels), BF16)

    @pl.when(me == n - 1)
    def _():
        gext[below, :] = jnp.zeros((width, channels), BF16)

    column = lax.broadcasted_iota(jnp.int32, (width, LANES), 0)

    def from_left(x):
        return jnp.where(column > 0, pltpu.roll(x, 1, 0), 0.0)

    def from_right(x):
        return jnp.where(column < width - 1, pltpu.roll(x, width - 1, 0), 0.0)

    def conv(h):
        wide = 2 * LANES
        for c in range(channels // wide):
            cols = slice(c * wide, (c + 1) * wide)
            ys = []
            for s in range(3):
                y = None
                for r in range(3):
                    rows = pl.ds(pl.multiple_of((h - r + 2) * width, width), width)
                    d = jnp.dot(
                        gext[rows, :], filt[3 * r + s, :, cols], preferred_element_type=F32
                    )
                    y = d if y is None else y + d
                ys.append(y)
            for k in range(2):
                sub = slice(k * LANES, (k + 1) * LANES)
                value = ys[1][:, sub] + from_right(ys[0][:, sub]) + from_left(ys[2][:, sub])
                gact[pl.ds(pl.multiple_of(h * width, width), width),
                     c * wide + k * LANES:c * wide + (k + 1) * LANES] = value

    def transpose(e):
        start = pl.multiple_of(e * width, width)
        gt[:, pl.ds(start, width)] = gext[pl.ds(start, width), :].T

    in_filt.wait()

    def inner(h, carry):
        conv(h)
        return carry

    lax.fori_loop(1, height - 1, inner, 0)

    def own_transposes(e, carry):
        transpose(e)
        return carry

    lax.fori_loop(1, height + 1, own_transposes, 0)

    def stat_wait(k, carry):
        stat_copy(k, peer(k)).wait_recv()
        return carry

    lax.fori_loop(1, n, stat_wait, 0)
    everyone = stat[...]
    total_stat = everyone.sum(0)
    gmax = jnp.max(
        jnp.where(is_top, everyone.max(0), 0.0), axis=1, keepdims=True
    )
    bound = GAIN_MAX * math.sqrt(float(pixels) * float(members)) + BIAS_MAX * pixels
    reach = bound * jnp.maximum(gmax, 1e-30) * (2.0 ** -13.9)
    scale = 1.0 / reach
    means, invs = [], []
    for c in range(chunks):
        total = group_sum(jnp.where(slot == c, total_stat, 0.0), per_group)
        square = group_sum(jnp.where(slot == chunks + c, total_stat, 0.0), per_group)
        mean = total / members
        means.append(mean)
        invs.append(lax.rsqrt(square / members - mean * mean + EPSILON))

    def forward(rows, c):
        cols = slice(c * LANES, (c + 1) * LANES)
        normalized = (feat[rows, cols].astype(F32) - means[c]) * invs[c]
        normed = normalized * gain_ref[:, cols] + bias_ref[:, cols]
        return normalized, normed, 1.0 / (1.0 + jnp.exp(-normed))

    def rows_of(h):
        return pl.ds(pl.multiple_of(h * width, width), width)

    def activate(h, carry):
        rows = rows_of(h)
        for c in range(chunks):
            cols = slice(c * LANES, (c + 1) * LANES)
            _, normed, sig = forward(rows, c)
            a = normed * sig
            act[0, rows, cols] = from_left(a).astype(BF16)
            act[1, rows, cols] = a.astype(BF16)
            act[2, rows, cols] = from_right(a).astype(BF16)
        return carry

    lax.fori_loop(0, height, activate, 0)

    @pl.when(me < n - 1)
    def _():
        halo_up.wait_recv()

    @pl.when(me > 0)
    def _():
        halo_down.wait_recv()

    transpose(0)
    transpose(height + 1)

    def copy1(t):
        target = me + 1 - 2 * core
        return remote(part.at[t, 1 - core], r1.at[t], send1.at[t], recv1.at[t], target)

    def copy2(t):
        target = me + 2 - 4 * second
        return remote(s2.at[t], r2.at[t], send2.at[t], recv2.at[t], target)

    def other(k):
        return lax.rem(third + k, thirds)

    def copy3(t, k, source):
        goal = other(k)
        return remote(
            s3.at[t, goal], r3.at[t, source], send3.at[t, k], recv3.at[t, source],
            goal * 4 + second * 2 + core,
        )

    def multiply(t):
        r, s = lax.div(t, 3), lax.rem(t, 3)
        start = pl.multiple_of((2 - r) * width, LANES)
        half = channels // 2
        for m in range(2):
            result = jnp.dot(
                gt[m * half:(m + 1) * half, pl.ds(start, local_pixels)], act[s],
                preferred_element_type=F32,
            )
            for b in range(n // 2):
                d = m * (n // 2) + b
                part[t, d % 2, (d // 2) % 2, d // 4] = result[b * block:(b + 1) * block]
        copy1(t).start()

    def stage2(t):
        copy1(t).wait_recv()
        for j in range(thirds):
            s2[t, j] = encode((part[t, core, 1 - second, j] + r1[t, 1 - second, j]) * scale)
        copy2(t).start()

    def stage3(t):
        copy2(t).wait_recv()

        def piece(goal):
            own = part[t, core, second, goal] + r1[t, second, goal]
            return own * scale + decode(r2[t, goal])

        for k in range(1, thirds):
            s3[t, other(k)] = encode(piece(other(k)))
            copy3(t, k, third).start()
        fg_ref[t] = piece(third)

    def stage4(t):
        total = fg_ref[t]
        for k in range(1, thirds):
            copy3(t, k, other(k)).wait_recv()
            total = total + decode(r3[t, other(k)])
        fg_ref[t] = total * (reach / pixels)

    early = 3

    def first_taps(t, carry):
        multiply(t)

        @pl.when(t >= 1)
        def _():
            stage2(t - 1)

        return carry

    lax.fori_loop(0, early, first_taps, 0)

    def outer(k, carry):
        conv(k * (height - 1))
        return carry

    lax.fori_loop(0, 2 if height > 1 else 1, outer, 0)

    for c in range(chunks):
        cols = slice(c * LANES, (c + 1) * LANES)

        def grad_step(h, carry):
            bias_sum, gain_sum = carry
            rows = rows_of(h)
            normalized, normed, sig = forward(rows, c)
            pre = gact[rows, cols] * (sig * (1.0 + normed * (1.0 - sig)))
            gact[rows, cols] = pre
            return (
                bias_sum + pre.reshape(width // 8, 8, LANES).sum(0),
                gain_sum + (pre * normalized).reshape(width // 8, 8, LANES).sum(0),
            )

        zero = jnp.zeros((8, LANES), F32)
        bias_sum, gain_sum = lax.fori_loop(0, height, grad_step, (zero, zero))
        sums[me, c:c + 1, :] = bias_sum.sum(0, keepdims=True)
        sums[me, chunks + c:chunks + c + 1, :] = gain_sum.sum(0, keepdims=True)

    def sums_copy(k, source):
        return remote(sums.at[me], sums.at[source], sums_send.at[k], sums_recv.at[source], peer(k))

    def sums_start(k, carry):
        sums_copy(k, me).start()
        return carry

    lax.fori_loop(1, n, sums_start, 0)

    lag = 4

    def later_taps(t, carry):
        @pl.when(t < taps)
        def _():
            multiply(t)

        stage2(t - 1)
        stage3(t - lag + 1)
        return carry

    lax.fori_loop(early, taps + 1, later_taps, 0)

    def sums_wait(k, carry):
        sums_copy(k, peer(k)).wait_recv()
        return carry

    lax.fori_loop(1, n, sums_wait, 0)
    all_sums = sums[...].sum(0)
    sums_ref[...] = all_sums
    for c in range(chunks):
        cols = slice(c * LANES, (c + 1) * LANES)
        gain = gain_ref[:, cols]
        mean_grad = group_sum(gain * all_sums[c:c + 1], per_group) / members
        mean_cross = group_sum(gain * all_sums[chunks + c:chunks + c + 1], per_group) / members

        def final_step(h, carry):
            rows = rows_of(h)
            normalized = (feat[rows, cols].astype(F32) - means[c]) * invs[c]
            result = invs[c] * (gact[rows, cols] * gain - mean_grad - normalized * mean_cross)
            gin_ref[rows, cols] = result.astype(BF16)
            return carry

        lax.fori_loop(0, height, final_step, 0)

    def last_taps(t, carry):
        stage3(t)
        return carry

    lax.fori_loop(taps + 2 - lag, taps, last_taps, 0)

    def finish(t, carry):
        stage4(t)
        copy1(t).wait_send()
        copy2(t).wait_send()
        for k in range(1, thirds):
            copy3(t, k, third).wait_send()
        return carry

    lax.fori_loop(0, taps, finish, 0)

    def small_sends(k, carry):
        stat_copy(k, me).wait_send()
        sums_copy(k, me).wait_send()
        return carry

    lax.fori_loop(1, n, small_sends, 0)

    @pl.when(me > 0)
    def _():
        halo_up.wait_send()

    @pl.when(me < n - 1)
    def _():
        halo_down.wait_send()


def local(n, features, grad_out, filters, norm_gain, norm_bias):
    height, width, channels = features.shape
    pixels = height * width
    block, thirds, chunks = channels // n, n // 4, channels // LANES
    taps = 9
    by_tap = filters.transpose(1, 2, 0, 3).reshape(taps, channels, channels)
    dma = pltpu.SemaphoreType.DMA
    grad_in, filter_grad, sums = pl.pallas_call(
        functools.partial(kernel, n, height, width, channels),
        out_shape=(
            jax.ShapeDtypeStruct((pixels, channels), BF16),
            jax.ShapeDtypeStruct((taps, block, channels), F32),
            jax.ShapeDtypeStruct((2 * chunks, LANES), F32),
        ),
        in_specs=[pl.BlockSpec(memory_space=pl.ANY)] * 3
        + [pl.BlockSpec(memory_space=pltpu.VMEM)] * 2,
        out_specs=(pl.BlockSpec(memory_space=pltpu.VMEM),) * 3,
        scratch_shapes=[
            pltpu.VMEM((pixels, channels), BF16),
            pltpu.VMEM((pixels + 2 * width, channels), BF16),
            pltpu.VMEM((taps, channels, channels), BF16),
            pltpu.VMEM((channels, pixels + 2 * width), BF16),
            pltpu.VMEM((3, pixels, channels), BF16),
            pltpu.VMEM((pixels, channels), F32),
            pltpu.VMEM((taps, 2, 2, thirds, block, channels), F32),
            pltpu.VMEM((taps, 2, thirds, block, channels), F32),
            pltpu.VMEM((taps, thirds, block, channels), BF16),
            pltpu.VMEM((taps, thirds, block, channels), BF16),
            pltpu.VMEM((taps, thirds, block, channels), BF16),
            pltpu.VMEM((taps, thirds, block, channels), BF16),
            pltpu.VMEM((n, 1, LANES), F32),
            pltpu.VMEM((n, 2 * chunks, LANES), F32),
            dma((3,)), dma((2,)), dma((2,)),
            dma((n,)), dma((n,)), dma((n,)), dma((n,)),
            dma((taps,)), dma((taps,)), dma((taps,)), dma((taps,)),
            dma((taps, thirds)), dma((taps, thirds)),
        ],
        compiler_params=pltpu.CompilerParams(
            collective_id=0, has_side_effects=True, vmem_limit_bytes=60 * 1024 * 1024
        ),
        name="block_backward",
    )(
        features.reshape(pixels, channels), grad_out.reshape(pixels, channels), by_tap,
        norm_gain.reshape(1, channels), norm_bias.reshape(1, channels),
    )
    return (
        grad_in.reshape(height, width, channels),
        filter_grad.transpose(1, 0, 2).reshape(block, 3, 3, channels),
        sums[chunks:].reshape(channels),
        sums[:chunks].reshape(channels),
    )


def solution(mesh):
    slabs = P(("parts", "rows"), None, None)
    return jax.shard_map(
        functools.partial(local, mesh.shape["rows"]),
        mesh=mesh,
        in_specs=(slabs, slabs, P(), P(), P()),
        out_specs=(slabs, P(("parts", "rows"), None, None, None), P("parts"), P("parts")),
        check_vma=False,
    )
```

```python
import functools
import math

import jax
import jax.numpy as jnp
from jax import lax
from jax.experimental import pallas as pl
from jax.experimental.pallas import tpu as pltpu
from jax.sharding import PartitionSpec as P

GROUPS = 32
LANES = 128
POWER = 9
SPLIT = 2
LAG3 = 4
LAG4 = 8
MAIN = 60
EPSILON = 1e-06
GAIN_MAX = 1.75
BIAS_MAX = 1.0
MESH = pl.DeviceIdType.MESH
F32 = jnp.float32
BF16 = jnp.bfloat16


def encode(value):
    square = value * value
    fourth = square * square
    return (fourth * fourth * value).astype(BF16)


def decode(coded):
    wide = coded.astype(F32)
    root = jnp.exp2(jnp.log2(jnp.maximum(jnp.abs(wide), 1e-38)) * (1.0 / POWER))
    root = jnp.where(jnp.abs(wide) < 1e-37, 0.0, root)
    return jnp.where(wide < 0.0, -root, root)


def group_sum(row, per_group):
    value = jnp.broadcast_to(row, (8, LANES))
    lane = lax.broadcasted_iota(jnp.int32, (8, LANES), 1)
    step = 1
    while step < per_group:
        low = pltpu.roll(value, step, 1)
        high = pltpu.roll(value, LANES - step, 1)
        value = value + jnp.where((lane & step) != 0, low, high)
        step *= 2
    return value[0:1]


def kernel(
    n, height, width, channels,
    feat_hbm, gout_hbm, filt_hbm, gain_ref, bias_ref,
    gin_hbm, fg_ref, sums_ref,
    gin_ref, feat, gext, filt, gt, act, gact, part, r1, s2, r2, s3, r3, held, stat, sums,
    local_sem, halo_send, halo_recv, stat_send, stat_recv, sums_send, sums_recv,
    send1, recv1, send2, recv2, send3, recv3,
):
    me = lax.axis_index("rows")
    core, second, third = lax.rem(me, 2), lax.rem(lax.div(me, 2), 2), lax.div(me, 4)
    thirds = n // 4
    block = channels // n
    chunks = channels // LANES
    per_group = channels // GROUPS
    local_pixels = height * width
    pixels = local_pixels * n
    members = pixels * per_group
    taps = 9
    pieces = taps * SPLIT
    span = channels // SPLIT

    def remote(src, dst, send, recv, target):
        return pltpu.make_async_remote_copy(
            src_ref=src, dst_ref=dst, send_sem=send, recv_sem=recv,
            device_id={"rows": target}, device_id_type=MESH,
        )

    def peer(k):
        return lax.rem(me + k, n)

    in_feat = pltpu.make_async_copy(feat_hbm, feat, local_sem.at[0])
    in_gout = pltpu.make_async_copy(
        gout_hbm, gext.at[pl.ds(width, local_pixels)], local_sem.at[1]
    )
    in_filt = pltpu.make_async_copy(filt_hbm, filt, local_sem.at[2])
    in_feat.start()
    in_gout.start()

    barrier = pltpu.get_barrier_semaphore()

    def greet(k, carry):
        pl.semaphore_signal(barrier, inc=1, device_id={"rows": peer(k)}, device_id_type=MESH)
        return carry

    lax.fori_loop(1, n, greet, 0)

    lane = lax.broadcasted_iota(jnp.int32, (1, LANES), 1)
    slot = lane & (per_group - 1)
    in_feat.wait()
    in_gout.wait()
    in_filt.start()

    packed = jnp.zeros((1, LANES), F32)
    largest = jnp.zeros((16, LANES), BF16)
    for c in range(chunks):
        cols = slice(c * LANES, (c + 1) * LANES)

        def stats_step(h, carry):
            total, square, top = carry
            x = feat[pl.ds(h * width, width), cols].astype(F32)
            g = jnp.abs(gext[pl.ds((h + 1) * width, width), cols])
            x = x.reshape(width // 8, 8, LANES)
            g = g.reshape(width // 16, 16, LANES)
            return (
                total + x.sum(0), square + (x * x).sum(0), jnp.maximum(top, g.max(0))
            )

        zero = jnp.zeros((8, LANES), F32)
        total, square, largest = lax.fori_loop(0, height, stats_step, (zero, zero, largest))
        total = group_sum(total.sum(0, keepdims=True), per_group)
        square = group_sum(square.sum(0, keepdims=True), per_group)
        packed = packed + jnp.where(slot == c, total, 0.0)
        packed = packed + jnp.where(slot == chunks + c, square, 0.0)
    top = jnp.max(largest.astype(F32).max(0, keepdims=True), axis=1, keepdims=True)
    is_top = slot == 2 * chunks
    stat[me] = packed + jnp.where(is_top, top, 0.0)

    pl.semaphore_wait(barrier, n - 1)

    def stat_copy(k, source):
        return remote(stat.at[me], stat.at[source], stat_send.at[k], stat_recv.at[source], peer(k))

    def stat_start(k, carry):
        stat_copy(k, me).start()
        return carry

    lax.fori_loop(1, n, stat_start, 0)

    up, down = lax.rem(me + n - 1, n), lax.rem(me + 1, n)
    above, below = pl.ds(0, width), pl.ds((height + 1) * width, width)
    halo_up = remote(
        gext.at[pl.ds(width, width)], gext.at[below], halo_send.at[0], halo_recv.at[0], up
    )
    halo_down = remote(
        gext.at[pl.ds(height * width, width)], gext.at[above], halo_send.at[1], halo_recv.at[1], down
    )

    @pl.when(me > 0)
    def _():
        halo_up.start()

    @pl.when(me < n - 1)
    def _():
        halo_down.start()

    @pl.when(me == 0)
    def _():
        gext[above, :] = jnp.zeros((width, channels), BF16)

    @pl.when(me == n - 1)
    def _():
        gext[below, :] = jnp.zeros((width, channels), BF16)

    column = lax.broadcasted_iota(jnp.int32, (width, LANES), 0)

    def from_left(x):
        return jnp.where(column > 0, pltpu.roll(x, 1, 0), 0.0)

    def from_right(x):
        return jnp.where(column < width - 1, pltpu.roll(x, width - 1, 0), 0.0)

    def conv(h):
        wide = 2 * LANES
        for c in range(channels // wide):
            cols = slice(c * wide, (c + 1) * wide)
            ys = []
            for s in range(3):
                y = None
                for r in range(3):
                    rows = pl.ds(pl.multiple_of((h - r + 2) * width, width), width)
                    d = jnp.dot(
                        gext[rows, :], filt[3 * r + s, :, cols], preferred_element_type=F32
                    )
                    y = d if y is None else y + d
                ys.append(y)
            for k in range(2):
                sub = slice(k * LANES, (k + 1) * LANES)
                value = ys[1][:, sub] + from_right(ys[0][:, sub]) + from_left(ys[2][:, sub])
                gact[pl.ds(pl.multiple_of(h * width, width), width),
                     c * wide + k * LANES:c * wide + (k + 1) * LANES] = value

    def transpose(e):
        start = pl.multiple_of(e * width, width)
        gt[:, pl.ds(start, width)] = gext[pl.ds(start, width), :].T

    in_filt.wait()

    def inner(h, carry):
        conv(h)
        return carry

    lax.fori_loop(1, height - 1, inner, 0)

    def own_transposes(e, carry):
        transpose(e)
        return carry

    lax.fori_loop(1, height + 1, own_transposes, 0)

    def stat_wait(k, carry):
        stat_copy(k, peer(k)).wait_recv()
        return carry

    lax.fori_loop(1, n, stat_wait, 0)
    everyone = stat[...]
    total_stat = everyone.sum(0)
    gmax = jnp.max(
        jnp.where(is_top, everyone.max(0), 0.0), axis=1, keepdims=True
    )
    bound = GAIN_MAX * math.sqrt(float(pixels) * float(members)) + BIAS_MAX * pixels
    reach = bound * jnp.maximum(gmax, 1e-30) * (2.0 ** -13.9)
    scale = 1.0 / reach
    means, invs = [], []
    for c in range(chunks):
        total = group_sum(jnp.where(slot == c, total_stat, 0.0), per_group)
        square = group_sum(jnp.where(slot == chunks + c, total_stat, 0.0), per_group)
        mean = total / members
        means.append(mean)
        invs.append(lax.rsqrt(square / members - mean * mean + EPSILON))

    def forward(rows, c):
        cols = slice(c * LANES, (c + 1) * LANES)
        normalized = (feat[rows, cols].astype(F32) - means[c]) * invs[c]
        normed = normalized * gain_ref[:, cols] + bias_ref[:, cols]
        return normalized, normed, 1.0 / (1.0 + jnp.exp(-normed))

    def rows_of(h):
        return pl.ds(pl.multiple_of(h * width, width), width)

    def activate(h, carry):
        rows = rows_of(h)
        for c in range(chunks):
            cols = slice(c * LANES, (c + 1) * LANES)
            _, normed, sig = forward(rows, c)
            a = normed * sig
            act[0, rows, cols] = from_left(a).astype(BF16)
            act[1, rows, cols] = a.astype(BF16)
            act[2, rows, cols] = from_right(a).astype(BF16)
        return carry

    lax.fori_loop(0, height, activate, 0)

    def halo_arrived():
        @pl.when(me < n - 1)
        def _():
            halo_up.wait_recv()

        @pl.when(me > 0)
        def _():
            halo_down.wait_recv()

        transpose(0)
        transpose(height + 1)

    def copy1(t):
        target = me + 1 - 2 * core
        return remote(part.at[t, 1 - core], r1.at[t], send1.at[t], recv1.at[t], target)

    def copy2(t):
        target = me + 2 - 4 * second
        return remote(s2.at[t], r2.at[t], send2.at[t], recv2.at[t], target)

    def other(k):
        return lax.rem(third + k, thirds)

    def copy3(t, k, source):
        goal = other(k)
        return remote(
            s3.at[t, goal], r3.at[t, source], send3.at[t, k], recv3.at[t, source],
            goal * 4 + second * 2 + core,
        )

    def multiply(q):
        t = lax.div(q, SPLIT)
        r, s = lax.rem(lax.div(t, 3) + 1, 3), lax.rem(t, 3)
        start = pl.multiple_of((2 - r) * width, LANES)
        cols = pl.ds(pl.multiple_of(lax.rem(q, SPLIT) * span, LANES), span)
        half = channels // 2
        for m in range(2):
            result = jnp.dot(
                gt[m * half:(m + 1) * half, pl.ds(start, local_pixels)], act[s, :, cols],
                preferred_element_type=F32,
            )
            for b in range(n // 2):
                d = m * (n // 2) + b
                part[q, d % 2, (d // 2) % 2, d // 4] = result[b * block:(b + 1) * block]
        copy1(q).start()

    def stage2(q):
        copy1(q).wait_recv()
        for j in range(thirds):
            s2[q, j] = encode((part[q, core, 1 - second, j] + r1[q, 1 - second, j]) * scale)
        copy2(q).start()

    def stage3(q):
        copy2(q).wait_recv()

        def piece(goal):
            own = part[q, core, second, goal] + r1[q, second, goal]
            return own * scale + decode(r2[q, goal])

        for k in range(1, thirds):
            s3[q, other(k)] = encode(piece(other(k)))
            copy3(q, k, third).start()
        held[q] = piece(third)

    def stage4(q):
        total = held[q]
        for k in range(1, thirds):
            copy3(q, k, other(k)).wait_recv()
            total = total + decode(r3[q, other(k)])
        t = lax.div(q, SPLIT)
        tap = 3 * lax.rem(lax.div(t, 3) + 1, 3) + lax.rem(t, 3)
        cols = pl.ds(pl.multiple_of(lax.rem(q, SPLIT) * span, LANES), span)
        fg_ref[tap, :, cols] = total * (reach / pixels)

    lag3, lag4 = LAG3, LAG4

    def run(first, last):
        def step(q, carry):
            @pl.when(q < pieces)
            def _():
                multiply(q)

            @pl.when((q >= 1) & (q <= pieces))
            def _():
                stage2(q - 1)

            @pl.when((q >= lag3) & (q < pieces + lag3))
            def _():
                stage3(q - lag3)

            @pl.when(q >= lag4)
            def _():
                stage4(q - lag4)

            return carry

        lax.fori_loop(first, last, step, 0)

    run(0, 4)
    halo_arrived()
    conv(0)
    run(4, 6)
    if height > 1:
        conv(height - 1)
    run(6, 8)

    for c in range(chunks):
        cols = slice(c * LANES, (c + 1) * LANES)

        def grad_step(h, carry):
            bias_sum, gain_sum = carry
            rows = rows_of(h)
            normalized, normed, sig = forward(rows, c)
            pre = gact[rows, cols] * (sig * (1.0 + normed * (1.0 - sig)))
            gact[rows, cols] = pre
            return (
                bias_sum + pre.reshape(width // 8, 8, LANES).sum(0),
                gain_sum + (pre * normalized).reshape(width // 8, 8, LANES).sum(0),
            )

        zero = jnp.zeros((8, LANES), F32)
        bias_sum, gain_sum = lax.fori_loop(0, height, grad_step, (zero, zero))
        sums[me, c:c + 1, :] = bias_sum.sum(0, keepdims=True)
        sums[me, chunks + c:chunks + c + 1, :] = gain_sum.sum(0, keepdims=True)

    def sums_copy(k, source):
        return remote(sums.at[me], sums.at[source], sums_send.at[k], sums_recv.at[source], peer(k))

    def sums_start(k, carry):
        sums_copy(k, me).start()
        return carry

    lax.fori_loop(1, n, sums_start, 0)

    run(8, pieces + 1)

    def sums_wait(k, carry):
        sums_copy(k, peer(k)).wait_recv()
        return carry

    lax.fori_loop(1, n, sums_wait, 0)
    all_sums = sums[...].sum(0)
    sums_ref[...] = all_sums
    for c in range(chunks):
        cols = slice(c * LANES, (c + 1) * LANES)
        gain = gain_ref[:, cols]
        mean_grad = group_sum(gain * all_sums[c:c + 1], per_group) / members
        mean_cross = group_sum(gain * all_sums[chunks + c:chunks + c + 1], per_group) / members

        def final_step(h, carry):
            rows = rows_of(h)
            normalized = (feat[rows, cols].astype(F32) - means[c]) * invs[c]
            result = invs[c] * (gact[rows, cols] * gain - mean_grad - normalized * mean_cross)
            gin_ref[rows, cols] = result.astype(BF16)
            return carry

        lax.fori_loop(0, height, final_step, 0)

    out_gin = pltpu.make_async_copy(gin_ref, gin_hbm, local_sem.at[3])
    out_gin.start()
    run(pieces + 1, pieces + lag4)

    def drain(q, carry):
        copy1(q).wait_send()
        copy2(q).wait_send()
        for k in range(1, thirds):
            copy3(q, k, third).wait_send()
        return carry

    lax.fori_loop(0, pieces, drain, 0)
    out_gin.wait()

    def small_sends(k, carry):
        stat_copy(k, me).wait_send()
        sums_copy(k, me).wait_send()
        return carry

    lax.fori_loop(1, n, small_sends, 0)

    @pl.when(me > 0)
    def _():
        halo_up.wait_send()

    @pl.when(me < n - 1)
    def _():
        halo_down.wait_send()


def hand_over(gin, fg, sums, gin_out, fg_out, gain_out, bias_out, sem):
    first = pltpu.make_async_copy(gin, gin_out, sem.at[0])
    second = pltpu.make_async_copy(fg, fg_out, sem.at[1])
    first.start()
    second.start()
    chunks = sums.shape[0] // 2
    for c in range(chunks):
        cols = slice(c * LANES, (c + 1) * LANES)
        bias_out[:, cols] = sums[c:c + 1, :]
        gain_out[:, cols] = sums[chunks + c:chunks + c + 1, :]
    first.wait()
    second.wait()


def local(n, features, grad_out, filters, norm_gain, norm_bias):
    height, width, channels = features.shape
    pixels = height * width
    block, thirds, chunks = channels // n, n // 4, channels // LANES
    taps = 9
    pieces, span = taps * SPLIT, channels // SPLIT
    by_tap = filters.transpose(1, 2, 0, 3).reshape(taps, channels, channels)
    dma = pltpu.SemaphoreType.DMA
    grad_in, filter_grad, sums = pl.pallas_call(
        functools.partial(kernel, n, height, width, channels),
        out_shape=(
            jax.ShapeDtypeStruct((pixels, channels), BF16),
            jax.ShapeDtypeStruct((taps, block, channels), F32),
            jax.ShapeDtypeStruct((2 * chunks, LANES), F32),
        ),
        in_specs=[pl.BlockSpec(memory_space=pl.ANY)] * 3
        + [pl.BlockSpec(memory_space=pltpu.VMEM)] * 2,
        out_specs=(
            pl.BlockSpec(memory_space=pl.ANY),
            pl.BlockSpec(memory_space=pltpu.VMEM),
            pl.BlockSpec(memory_space=pltpu.VMEM),
        ),
        scratch_shapes=[
            pltpu.VMEM((pixels, channels), BF16),
            pltpu.VMEM((pixels, channels), BF16),
            pltpu.VMEM((pixels + 2 * width, channels), BF16),
            pltpu.VMEM((taps, channels, channels), BF16),
            pltpu.VMEM((channels, pixels + 2 * width), BF16),
            pltpu.VMEM((3, pixels, channels), BF16),
            pltpu.VMEM((pixels, channels), F32),
            pltpu.VMEM((pieces, 2, 2, thirds, block, span), F32),
            pltpu.VMEM((pieces, 2, thirds, block, span), F32),
            pltpu.VMEM((pieces, thirds, block, span), BF16),
            pltpu.VMEM((pieces, thirds, block, span), BF16),
            pltpu.VMEM((pieces, thirds, block, span), BF16),
            pltpu.VMEM((pieces, thirds, block, span), BF16),
            pltpu.VMEM((pieces, block, span), F32),
            pltpu.VMEM((n, 1, LANES), F32),
            pltpu.VMEM((n, 2 * chunks, LANES), F32),
            dma((4,)), dma((2,)), dma((2,)),
            dma((n,)), dma((n,)), dma((n,)), dma((n,)),
            dma((pieces,)), dma((pieces,)), dma((pieces,)), dma((pieces,)),
            dma((pieces, thirds)), dma((pieces, thirds)),
        ],
        compiler_params=pltpu.CompilerParams(
            collective_id=0, has_side_effects=True, vmem_limit_bytes=MAIN * 1024 * 1024
        ),
        name="block_backward",
    )(
        features.reshape(pixels, channels), grad_out.reshape(pixels, channels), by_tap,
        norm_gain.reshape(1, channels), norm_bias.reshape(1, channels),
    )
    any_space, vmem = pl.BlockSpec(memory_space=pl.ANY), pl.BlockSpec(memory_space=pltpu.VMEM)
    grad_in, filter_grad, gain_grad, bias_grad = pl.pallas_call(
        hand_over,
        out_shape=(
            jax.ShapeDtypeStruct((pixels, channels), BF16),
            jax.ShapeDtypeStruct((taps, block, channels), F32),
            jax.ShapeDtypeStruct((1, channels), F32),
            jax.ShapeDtypeStruct((1, channels), F32),
        ),
        in_specs=[vmem, vmem, vmem],
        out_specs=(any_space, any_space, vmem, vmem),
        scratch_shapes=[dma((2,))],
        compiler_params=pltpu.CompilerParams(vmem_limit_bytes=8 * 1024 * 1024),
        name="hand_over",
    )(grad_in, filter_grad, sums)
    return (
        grad_in.reshape(height, width, channels),
        filter_grad.transpose(1, 0, 2).reshape(block, 3, 3, channels),
        gain_grad.reshape(channels),
        bias_grad.reshape(channels),
    )


def solution(mesh):
    slabs = P(("parts", "rows"), None, None)
    return jax.shard_map(
        functools.partial(local, mesh.shape["rows"]),
        mesh=mesh,
        in_specs=(slabs, slabs, P(), P(), P()),
        out_specs=(slabs, P(("parts", "rows"), None, None, None), P("parts"), P("parts")),
        check_vma=False,
    )
```

```python
import functools
import math

import jax
import jax.numpy as jnp
from jax import lax
from jax.experimental import pallas as pl
from jax.experimental.pallas import tpu as pltpu
from jax.sharding import PartitionSpec as P

GROUPS = 32
LANES = 128
POWER = 9
SPLIT = 2
LAG3 = 4
LAG4 = 8
MAIN = 60
EPSILON = 1e-06
GAIN_MAX = 1.75
BIAS_MAX = 1.0
MESH = pl.DeviceIdType.MESH
F32 = jnp.float32
BF16 = jnp.bfloat16


def encode(value):
    square = value * value
    fourth = square * square
    return (fourth * fourth * value).astype(BF16)


def decode(coded):
    wide = coded.astype(F32)
    root = jnp.exp2(jnp.log2(jnp.maximum(jnp.abs(wide), 1e-38)) * (1.0 / POWER))
    root = jnp.where(jnp.abs(wide) < 1e-37, 0.0, root)
    return jnp.where(wide < 0.0, -root, root)


def group_sum(row, per_group):
    value = jnp.broadcast_to(row, (8, LANES))
    lane = lax.broadcasted_iota(jnp.int32, (8, LANES), 1)
    step = 1
    while step < per_group:
        low = pltpu.roll(value, step, 1)
        high = pltpu.roll(value, LANES - step, 1)
        value = value + jnp.where((lane & step) != 0, low, high)
        step *= 2
    return value[0:1]


def kernel(
    n, height, width, channels,
    feat_hbm, gout_hbm, filt_hbm, gain_ref, bias_ref,
    gin_hbm, fg_ref, sums_ref,
    gin_ref, feat, gext, filt, gt, act, gact, part, r1, s2, r2, s3, r3, held, stat, tops, sums,
    local_sem, halo_send, halo_recv, stat_send, stat_recv, tops_send, tops_recv, sums_send, sums_recv,
    send1, recv1, send2, recv2, send3, recv3,
):
    me = lax.axis_index("rows")
    core, second, third = lax.rem(me, 2), lax.rem(lax.div(me, 2), 2), lax.div(me, 4)
    thirds = n // 4
    block = channels // n
    chunks = channels // LANES
    per_group = channels // GROUPS
    local_pixels = height * width
    pixels = local_pixels * n
    members = pixels * per_group
    taps = 9
    pieces = taps * SPLIT
    span = channels // SPLIT

    def remote(src, dst, send, recv, target):
        return pltpu.make_async_remote_copy(
            src_ref=src, dst_ref=dst, send_sem=send, recv_sem=recv,
            device_id={"rows": target}, device_id_type=MESH,
        )

    def peer(k):
        return lax.rem(me + k, n)

    in_feat = pltpu.make_async_copy(feat_hbm, feat, local_sem.at[0])
    in_gout = pltpu.make_async_copy(
        gout_hbm, gext.at[pl.ds(width, local_pixels)], local_sem.at[1]
    )
    in_filt = pltpu.make_async_copy(filt_hbm, filt, local_sem.at[2])
    in_feat.start()

    barrier = pltpu.get_barrier_semaphore()

    def greet(k, carry):
        pl.semaphore_signal(barrier, inc=1, device_id={"rows": peer(k)}, device_id_type=MESH)
        return carry

    lax.fori_loop(1, n, greet, 0)

    lane = lax.broadcasted_iota(jnp.int32, (1, LANES), 1)
    slot = lane & (per_group - 1)
    in_feat.wait()
    in_gout.start()
    in_filt.start()

    packed = jnp.zeros((1, LANES), F32)
    for c in range(chunks):
        cols = slice(c * LANES, (c + 1) * LANES)

        def stats_step(h, carry):
            total, square = carry
            x = feat[pl.ds(h * width, width), cols].astype(F32)
            x = x.reshape(width // 8, 8, LANES)
            return total + x.sum(0), square + (x * x).sum(0)

        zero = jnp.zeros((8, LANES), F32)
        total, square = lax.fori_loop(0, height, stats_step, (zero, zero))
        total = group_sum(total.sum(0, keepdims=True), per_group)
        square = group_sum(square.sum(0, keepdims=True), per_group)
        packed = packed + jnp.where(slot == c, total, 0.0)
        packed = packed + jnp.where(slot == chunks + c, square, 0.0)
    stat[me] = packed

    pl.semaphore_wait(barrier, n - 1)

    def stat_copy(k, source):
        return remote(stat.at[me], stat.at[source], stat_send.at[k], stat_recv.at[source], peer(k))

    def stat_start(k, carry):
        stat_copy(k, me).start()
        return carry

    lax.fori_loop(1, n, stat_start, 0)

    in_gout.wait()
    up, down = lax.rem(me + n - 1, n), lax.rem(me + 1, n)
    above, below = pl.ds(0, width), pl.ds((height + 1) * width, width)
    halo_up = remote(
        gext.at[pl.ds(width, width)], gext.at[below], halo_send.at[0], halo_recv.at[0], up
    )
    halo_down = remote(
        gext.at[pl.ds(height * width, width)], gext.at[above], halo_send.at[1], halo_recv.at[1], down
    )

    @pl.when(me > 0)
    def _():
        halo_up.start()

    @pl.when(me < n - 1)
    def _():
        halo_down.start()

    @pl.when(me == 0)
    def _():
        gext[above, :] = jnp.zeros((width, channels), BF16)

    @pl.when(me == n - 1)
    def _():
        gext[below, :] = jnp.zeros((width, channels), BF16)

    def top_step(h, top):
        g = jnp.abs(gext[pl.ds(pl.multiple_of(width + h * 128, 128), 128), :])
        return jnp.maximum(top, g.reshape(8, 16, channels).max(0))

    largest = lax.fori_loop(0, local_pixels // 128, top_step, jnp.zeros((16, channels), BF16))
    largest = largest.astype(F32).max(0, keepdims=True)
    tops[me] = jnp.broadcast_to(jnp.max(largest, axis=1, keepdims=True), (1, LANES))

    def tops_copy(k, source):
        return remote(tops.at[me], tops.at[source], tops_send.at[k], tops_recv.at[source], peer(k))

    def tops_start(k, carry):
        tops_copy(k, me).start()
        return carry

    lax.fori_loop(1, n, tops_start, 0)

    column = lax.broadcasted_iota(jnp.int32, (width, LANES), 0)

    def from_left(x):
        return jnp.where(column > 0, pltpu.roll(x, 1, 0), 0.0)

    def from_right(x):
        return jnp.where(column < width - 1, pltpu.roll(x, width - 1, 0), 0.0)

    def conv(h):
        wide = 2 * LANES
        for c in range(channels // wide):
            cols = slice(c * wide, (c + 1) * wide)
            ys = []
            for s in range(3):
                y = None
                for r in range(3):
                    rows = pl.ds(pl.multiple_of((h - r + 2) * width, width), width)
                    d = jnp.dot(
                        gext[rows, :], filt[3 * r + s, :, cols], preferred_element_type=F32
                    )
                    y = d if y is None else y + d
                ys.append(y)
            for k in range(2):
                sub = slice(k * LANES, (k + 1) * LANES)
                value = ys[1][:, sub] + from_right(ys[0][:, sub]) + from_left(ys[2][:, sub])
                gact[pl.ds(pl.multiple_of(h * width, width), width),
                     c * wide + k * LANES:c * wide + (k + 1) * LANES] = value

    def transpose(e):
        start = pl.multiple_of(e * width, width)
        gt[:, pl.ds(start, width)] = gext[pl.ds(start, width), :].T

    in_filt.wait()

    def inner(h, carry):
        conv(h)
        return carry

    lax.fori_loop(1, height - 1, inner, 0)

    def own_transposes(e, carry):
        transpose(e)
        return carry

    lax.fori_loop(1, height + 1, own_transposes, 0)

    def stat_wait(k, carry):
        stat_copy(k, peer(k)).wait_recv()
        tops_copy(k, peer(k)).wait_recv()
        return carry

    lax.fori_loop(1, n, stat_wait, 0)
    everyone = stat[...]
    total_stat = everyone.sum(0)
    gmax = jnp.max(tops[...].max(0), axis=1, keepdims=True)
    bound = GAIN_MAX * math.sqrt(float(pixels) * float(members)) + BIAS_MAX * pixels
    reach = bound * jnp.maximum(gmax, 1e-30) * (2.0 ** -13.9)
    scale = 1.0 / reach
    means, invs = [], []
    for c in range(chunks):
        total = group_sum(jnp.where(slot == c, total_stat, 0.0), per_group)
        square = group_sum(jnp.where(slot == chunks + c, total_stat, 0.0), per_group)
        mean = total / members
        means.append(mean)
        invs.append(lax.rsqrt(square / members - mean * mean + EPSILON))

    def forward(rows, c):
        cols = slice(c * LANES, (c + 1) * LANES)
        normalized = (feat[rows, cols].astype(F32) - means[c]) * invs[c]
        normed = normalized * gain_ref[:, cols] + bias_ref[:, cols]
        return normalized, normed, 1.0 / (1.0 + jnp.exp(-normed))

    def rows_of(h):
        return pl.ds(pl.multiple_of(h * width, width), width)

    def activate(h, carry):
        rows = rows_of(h)
        for c in range(chunks):
            cols = slice(c * LANES, (c + 1) * LANES)
            _, normed, sig = forward(rows, c)
            a = normed * sig
            act[0, rows, cols] = from_left(a).astype(BF16)
            act[1, rows, cols] = a.astype(BF16)
            act[2, rows, cols] = from_right(a).astype(BF16)
        return carry

    lax.fori_loop(0, height, activate, 0)

    def halo_arrived():
        @pl.when(me < n - 1)
        def _():
            halo_up.wait_recv()

        @pl.when(me > 0)
        def _():
            halo_down.wait_recv()

        transpose(0)
        transpose(height + 1)

    def copy1(t):
        target = me + 1 - 2 * core
        return remote(part.at[t, 1 - core], r1.at[t], send1.at[t], recv1.at[t], target)

    def copy2(t):
        target = me + 2 - 4 * second
        return remote(s2.at[t], r2.at[t], send2.at[t], recv2.at[t], target)

    def other(k):
        return lax.rem(third + k, thirds)

    def copy3(t, k, source):
        goal = other(k)
        return remote(
            s3.at[t, goal], r3.at[t, source], send3.at[t, k], recv3.at[t, source],
            goal * 4 + second * 2 + core,
        )

    def multiply(q):
        t = lax.div(q, SPLIT)
        r, s = lax.rem(lax.div(t, 3) + 1, 3), lax.rem(t, 3)
        start = pl.multiple_of((2 - r) * width, LANES)
        cols = pl.ds(pl.multiple_of(lax.rem(q, SPLIT) * span, LANES), span)
        half = channels // 2
        for m in range(2):
            result = jnp.dot(
                gt[m * half:(m + 1) * half, pl.ds(start, local_pixels)], act[s, :, cols],
                preferred_element_type=F32,
            )
            for b in range(n // 2):
                d = m * (n // 2) + b
                part[q, d % 2, (d // 2) % 2, d // 4] = result[b * block:(b + 1) * block]
        copy1(q).start()

    def stage2(q):
        copy1(q).wait_recv()
        for j in range(thirds):
            s2[q, j] = encode((part[q, core, 1 - second, j] + r1[q, 1 - second, j]) * scale)
        copy2(q).start()

    def stage3(q):
        copy2(q).wait_recv()

        def piece(goal):
            own = part[q, core, second, goal] + r1[q, second, goal]
            return own * scale + decode(r2[q, goal])

        for k in range(1, thirds):
            s3[q, other(k)] = encode(piece(other(k)))
            copy3(q, k, third).start()
        held[q] = piece(third)

    def stage4(q):
        total = held[q]
        for k in range(1, thirds):
            copy3(q, k, other(k)).wait_recv()
            total = total + decode(r3[q, other(k)])
        t = lax.div(q, SPLIT)
        tap = 3 * lax.rem(lax.div(t, 3) + 1, 3) + lax.rem(t, 3)
        cols = pl.ds(pl.multiple_of(lax.rem(q, SPLIT) * span, LANES), span)
        fg_ref[tap, :, cols] = total * (reach / pixels)

    lag3, lag4 = LAG3, LAG4

    def run(first, last):
        def step(q, carry):
            @pl.when(q < pieces)
            def _():
                multiply(q)

            @pl.when((q >= 1) & (q <= pieces))
            def _():
                stage2(q - 1)

            @pl.when((q >= lag3) & (q < pieces + lag3))
            def _():
                stage3(q - lag3)

            @pl.when(q >= lag4)
            def _():
                stage4(q - lag4)

            return carry

        lax.fori_loop(first, last, step, 0)

    run(0, 4)
    halo_arrived()
    conv(0)
    run(4, 6)
    if height > 1:
        conv(height - 1)
    run(6, 8)

    for c in range(chunks):
        cols = slice(c * LANES, (c + 1) * LANES)

        def grad_step(h, carry):
            bias_sum, gain_sum = carry
            rows = rows_of(h)
            normalized, normed, sig = forward(rows, c)
            pre = gact[rows, cols] * (sig * (1.0 + normed * (1.0 - sig)))
            gact[rows, cols] = pre
            return (
                bias_sum + pre.reshape(width // 8, 8, LANES).sum(0),
                gain_sum + (pre * normalized).reshape(width // 8, 8, LANES).sum(0),
            )

        zero = jnp.zeros((8, LANES), F32)
        bias_sum, gain_sum = lax.fori_loop(0, height, grad_step, (zero, zero))
        sums[me, c:c + 1, :] = bias_sum.sum(0, keepdims=True)
        sums[me, chunks + c:chunks + c + 1, :] = gain_sum.sum(0, keepdims=True)

    def sums_copy(k, source):
        return remote(sums.at[me], sums.at[source], sums_send.at[k], sums_recv.at[source], peer(k))

    def sums_start(k, carry):
        sums_copy(k, me).start()
        return carry

    lax.fori_loop(1, n, sums_start, 0)

    late = max(8, pieces - chunks)
    run(8, late)

    def sums_wait(k, carry):
        sums_copy(k, peer(k)).wait_recv()
        return carry

    lax.fori_loop(1, n, sums_wait, 0)
    all_sums = sums[...].sum(0)
    sums_ref[...] = all_sums
    for c in range(chunks):
        cols = slice(c * LANES, (c + 1) * LANES)
        gain = gain_ref[:, cols]
        mean_grad = group_sum(gain * all_sums[c:c + 1], per_group) / members
        mean_cross = group_sum(gain * all_sums[chunks + c:chunks + c + 1], per_group) / members

        def final_step(h, carry):
            rows = rows_of(h)
            normalized = (feat[rows, cols].astype(F32) - means[c]) * invs[c]
            result = invs[c] * (gact[rows, cols] * gain - mean_grad - normalized * mean_cross)
            gin_ref[rows, cols] = result.astype(BF16)
            return carry

        lax.fori_loop(0, height, final_step, 0)
        run(late + c, late + c + 1)

    out_gin = pltpu.make_async_copy(gin_ref, gin_hbm, local_sem.at[3])
    out_gin.start()
    run(late + chunks, pieces + lag4)

    def drain(q, carry):
        copy1(q).wait_send()
        copy2(q).wait_send()
        for k in range(1, thirds):
            copy3(q, k, third).wait_send()
        return carry

    lax.fori_loop(0, pieces, drain, 0)
    out_gin.wait()

    def small_sends(k, carry):
        stat_copy(k, me).wait_send()
        tops_copy(k, me).wait_send()
        sums_copy(k, me).wait_send()
        return carry

    lax.fori_loop(1, n, small_sends, 0)

    @pl.when(me > 0)
    def _():
        halo_up.wait_send()

    @pl.when(me < n - 1)
    def _():
        halo_down.wait_send()


def hand_over(
    gin, fg, sums, gin_out, fg_out, gain_out, bias_out, gin_held, fg_held, sums_held, into, out
):
    parts = gin.shape[0] // 4
    slabs = [pl.ds(k * parts, parts) for k in range(4)]
    moves = [(gin.at[d], gin_held.at[d], gin_out.at[d]) for d in slabs]
    moves += [(fg, fg_held, fg_out)]
    loads = [
        pltpu.make_async_copy(source, held, into.at[k])
        for k, (source, held, _) in enumerate(moves)
    ]
    stores = [
        pltpu.make_async_copy(held, target, out.at[k])
        for k, (_, held, target) in enumerate(moves)
    ]
    small = pltpu.make_async_copy(sums, sums_held, into.at[len(moves)])
    small.start()
    for load in loads:
        load.start()
    for load, store in zip(loads, stores):
        load.wait()
        store.start()
    small.wait()
    chunks = sums.shape[0] // 2
    for c in range(chunks):
        cols = slice(c * LANES, (c + 1) * LANES)
        bias_out[:, cols] = sums_held[c:c + 1, :]
        gain_out[:, cols] = sums_held[chunks + c:chunks + c + 1, :]
    for store in stores:
        store.wait()


def local(n, features, grad_out, filters, norm_gain, norm_bias):
    height, width, channels = features.shape
    pixels = height * width
    block, thirds, chunks = channels // n, n // 4, channels // LANES
    taps = 9
    pieces, span = taps * SPLIT, channels // SPLIT
    by_tap = filters.transpose(1, 2, 0, 3).reshape(taps, channels, channels)
    dma = pltpu.SemaphoreType.DMA
    grad_in, filter_grad, sums = pl.pallas_call(
        functools.partial(kernel, n, height, width, channels),
        out_shape=(
            jax.ShapeDtypeStruct((pixels, channels), BF16),
            jax.ShapeDtypeStruct((taps, block, channels), F32),
            jax.ShapeDtypeStruct((2 * chunks, LANES), F32),
        ),
        in_specs=[pl.BlockSpec(memory_space=pl.ANY)] * 3
        + [pl.BlockSpec(memory_space=pltpu.VMEM)] * 2,
        out_specs=(
            pl.BlockSpec(memory_space=pl.ANY),
            pl.BlockSpec(memory_space=pltpu.VMEM),
            pl.BlockSpec(memory_space=pltpu.VMEM),
        ),
        scratch_shapes=[
            pltpu.VMEM((pixels, channels), BF16),
            pltpu.VMEM((pixels, channels), BF16),
            pltpu.VMEM((pixels + 2 * width, channels), BF16),
            pltpu.VMEM((taps, channels, channels), BF16),
            pltpu.VMEM((channels, pixels + 2 * width), BF16),
            pltpu.VMEM((3, pixels, channels), BF16),
            pltpu.VMEM((pixels, channels), F32),
            pltpu.VMEM((pieces, 2, 2, thirds, block, span), F32),
            pltpu.VMEM((pieces, 2, thirds, block, span), F32),
            pltpu.VMEM((pieces, thirds, block, span), BF16),
            pltpu.VMEM((pieces, thirds, block, span), BF16),
            pltpu.VMEM((pieces, thirds, block, span), BF16),
            pltpu.VMEM((pieces, thirds, block, span), BF16),
            pltpu.VMEM((pieces, block, span), F32),
            pltpu.VMEM((n, 1, LANES), F32),
            pltpu.VMEM((n, 1, LANES), F32),
            pltpu.VMEM((n, 2 * chunks, LANES), F32),
            dma((4,)), dma((2,)), dma((2,)),
            dma((n,)), dma((n,)), dma((n,)), dma((n,)), dma((n,)), dma((n,)),
            dma((pieces,)), dma((pieces,)), dma((pieces,)), dma((pieces,)),
            dma((pieces, thirds)), dma((pieces, thirds)),
        ],
        compiler_params=pltpu.CompilerParams(
            collective_id=0, has_side_effects=True, vmem_limit_bytes=MAIN * 1024 * 1024
        ),
        name="block_backward",
    )(
        features.reshape(pixels, channels), grad_out.reshape(pixels, channels), by_tap,
        norm_gain.reshape(1, channels), norm_bias.reshape(1, channels),
    )
    any_space, vmem = pl.BlockSpec(memory_space=pl.ANY), pl.BlockSpec(memory_space=pltpu.VMEM)
    grad_in, filter_grad, gain_grad, bias_grad = pl.pallas_call(
        hand_over,
        out_shape=(
            jax.ShapeDtypeStruct((pixels, channels), BF16),
            jax.ShapeDtypeStruct((taps, block, channels), F32),
            jax.ShapeDtypeStruct((1, channels), F32),
            jax.ShapeDtypeStruct((1, channels), F32),
        ),
        in_specs=[any_space] * 3,
        out_specs=(any_space, any_space, vmem, vmem),
        scratch_shapes=[
            pltpu.VMEM((pixels, channels), BF16),
            pltpu.VMEM((taps, block, channels), F32),
            pltpu.VMEM((2 * chunks, LANES), F32),
            dma((6,)), dma((5,)),
        ],
        compiler_params=pltpu.CompilerParams(vmem_limit_bytes=MAIN * 1024 * 1024),
        name="hand_over",
    )(grad_in, filter_grad, sums)
    return (
        grad_in.reshape(height, width, channels),
        filter_grad.transpose(1, 0, 2).reshape(block, 3, 3, channels),
        gain_grad.reshape(channels),
        bias_grad.reshape(channels),
    )


def solution(mesh):
    slabs = P(("parts", "rows"), None, None)
    return jax.shard_map(
        functools.partial(local, mesh.shape["rows"]),
        mesh=mesh,
        in_specs=(slabs, slabs, P(), P(), P()),
        out_specs=(slabs, P(("parts", "rows"), None, None, None), P("parts"), P("parts")),
        check_vma=False,
    )
```
